8 devices in a mesh: batch: 1 (over z), gz: 2 (over y), gy: 2 (over x), gx: 2 (over core).
Axes of the slice: x: 2, y: 2, z: 1, core: 2. Of those that a mesh axis runs over, the one named last changes fastest.
Arguments:
- rhs_grid: float32 [256, 256, 256], P(('batch', 'gz'), 'gy', 'gx')
- init_grid: float32 [256, 256, 256], P(('batch', 'gz'), 'gy', 'gx')
- coarse_inv: float32 [64, 64], replicated
Outputs:
- output: float32 [256, 256, 256], P(('batch', 'gz'), 'gy', 'gx')
All inputs are finite; a program needn't handle non-finite values.
Results may differ from the reference program's by a relative error of at most 0.001.
Values sent between devices are 32-bit elements.
A program may use at most 1 GiB of HBM per device.

```python
import jax
import jax.numpy as jnp
from jax import lax

COARSE = 4
LEVELS = 6
CYCLES = 2
SWEEPS = 2
MODES = 8
N = COARSE * 2 ** LEVELS
OMEGA = 2.0 / 3.0


def with_ghosts(iterate, axis_id):
    extent = iterate.shape[axis_id]
    first_face = lax.slice_in_dim(iterate, 0, 1, axis=axis_id)
    last_face = lax.slice_in_dim(iterate, extent - 1, extent, axis=axis_id)
    return jnp.concatenate([-first_face, iterate, -last_face], axis=axis_id)


def neighbour_sum(iterate):
    nbr_total = jnp.zeros_like(iterate)
    for axis_id in range(3):
        extent = iterate.shape[axis_id]
        padded = with_ghosts(iterate, axis_id)
        nbr_total = nbr_total + lax.slice_in_dim(padded, 0, extent, axis=axis_id) + lax.slice_in_dim(padded, 2, extent + 2, axis=axis_id)
    return nbr_total


def jacobi(iterate, source, edge_cells):
    return (1.0 - OMEGA) * iterate + (OMEGA / 6.0) * (source * (1.0 / (edge_cells * edge_cells)) + neighbour_sum(iterate))


def residual(iterate, source, edge_cells):
    return source - (6.0 * iterate - neighbour_sum(iterate)) * float(edge_cells * edge_cells)


def restrict(fine_grid):
    dim_z, dim_y, dim_x = fine_grid.shape
    return fine_grid.reshape(dim_z // 2, 2, dim_y // 2, 2, dim_x // 2, 2).mean(axis=(1, 3, 5))


def prolong(coarse):
    for axis_id in range(3):
        extent = coarse.shape[axis_id]
        padded = with_ghosts(coarse, axis_id)
        low_child = 0.75 * coarse + 0.25 * lax.slice_in_dim(padded, 0, extent, axis=axis_id)
        high_child = 0.75 * coarse + 0.25 * lax.slice_in_dim(padded, 2, extent + 2, axis=axis_id)
        new_shape = list(coarse.shape)
        new_shape[axis_id] = 2 * extent
        coarse = jnp.stack([low_child, high_child], axis=axis_id + 1).reshape(new_shape)
    return coarse


def vcycle(iterate, source, level_id, coarse_inv):
    if level_id == LEVELS:
        flat_rhs = source.reshape(-1)
        return jnp.dot(coarse_inv, flat_rhs, precision=lax.Precision.HIGHEST).reshape(source.shape)
    edge_cells = N // 2 ** level_id
    for sweep_id in range(SWEEPS):
        iterate = jacobi(iterate, source, edge_cells)
    coarse_rhs = restrict(residual(iterate, source, edge_cells))
    correction = vcycle(jnp.zeros_like(coarse_rhs), coarse_rhs, level_id + 1, coarse_inv)
    iterate = iterate + prolong(correction)
    for sweep_id in range(SWEEPS):
        iterate = jacobi(iterate, source, edge_cells)
    return iterate


def smooth_field(rand_key, extent):
    coeffs = jax.random.normal(rand_key, (MODES, MODES, MODES), jnp.float32)
    wavenum = jnp.arange(1, MODES + 1).astype(jnp.float32)
    weight = (wavenum[:, None, None] ** 2 + wavenum[None, :, None] ** 2 + wavenum[None, None, :] ** 2) ** -0.5
    centres = (jnp.arange(extent).astype(jnp.float32) + 0.5) / extent
    sine_table = jnp.sin(jnp.pi * wavenum[:, None] * centres[None, :])
    smooth = jnp.einsum('abc,ai,bj,ck->ijk', coeffs * weight, sine_table, sine_table, sine_table)
    return smooth / jnp.sqrt(jnp.mean(smooth * smooth))


def coarse_inverse(rand_key):
    scale_key, diag_key = jax.random.split(rand_key)
    cell_ids = jnp.arange(COARSE)
    line_diag = 2.0 + (cell_ids == 0).astype(jnp.float32) + (cell_ids == COARSE - 1).astype(jnp.float32)
    line_op = jnp.diag(line_diag) - jnp.eye(COARSE, k=1, dtype=jnp.float32) - jnp.eye(COARSE, k=-1, dtype=jnp.float32)
    identity = jnp.eye(COARSE, dtype=jnp.float32)
    laplace = (jnp.kron(jnp.kron(line_op, identity), identity) + jnp.kron(jnp.kron(identity, line_op), identity) + jnp.kron(jnp.kron(identity, identity), line_op)) * float(COARSE * COARSE)
    shift_scale = jax.random.uniform(scale_key, (), jnp.float32, 0.5, 1.5)
    shifts = 30.0 * shift_scale * jax.random.uniform(diag_key, (COARSE ** 3,), jnp.float32, 0.5, 1.5)
    return jnp.linalg.inv(laplace + jnp.diag(shifts))


def setup_inputs(seed: int = 0, part: int = 0) -> dict:
    key_list = jax.random.split(jax.random.key(seed), 5)
    rhs_smooth_key = jax.random.fold_in(key_list[0], part)
    rhs_noise_key = jax.random.fold_in(key_list[1], part)
    init_smooth_key = jax.random.fold_in(key_list[2], part)
    init_noise_key = jax.random.fold_in(key_list[3], part)
    rhs_grid = 30.0 * smooth_field(rhs_smooth_key, N) + 10.0 * jax.random.normal(rhs_noise_key, (N, N, N), jnp.float32)
    init_grid = smooth_field(init_smooth_key, N) + 0.5 * jax.random.normal(init_noise_key, (N, N, N), jnp.float32)
    coarse_inv = coarse_inverse(key_list[4])
    return {'rhs_grid': rhs_grid, 'init_grid': init_grid, 'coarse_inv': coarse_inv}


def reference(rhs_grid, init_grid, coarse_inv):
    iterate = init_grid
    for cycle_id in range(CYCLES):
        iterate = vcycle(iterate, rhs_grid, 0, coarse_inv)
    return iterate
```

```python
import functools

import jax
import jax.numpy as jnp
from jax import lax
from jax.experimental import pallas as pl
from jax.experimental.pallas import tpu as pltpu
from jax.sharding import PartitionSpec as P

MESH = pl.DeviceIdType.MESH
F32 = jnp.float32
NINTH = 1.0 / 9.0
H = 6
G3 = 4
CYCLES = 2
DU, DF, DV = 3, 4, 5
SUB, LANES = 8, 128
NEAR, FAR = 0.75, 0.25
COARSE = 4
VREGS = 72
BLOCK0 = 136
BLOCK1 = 136
BLOCKP = 64


def _loop(lo, count, step, body):
    assert count % step == 0

    def run(i, carry):
        body(lo + i * step)
        return carry

    if count == step:
        body(lo)
    else:
        lax.fori_loop(0, count // step, run, 0)


def _iota(shape, axis):
    return lax.broadcasted_iota(jnp.int32, shape, len(shape) + axis)


def _ysum(load, lo, n, total, v, last_row=7):
    sub = _iota((v.shape[0], SUB, LANES), -2)
    if lo == 0:
        ym = jnp.where(sub == 0, -v[:, :SUB], pltpu.roll(v[:, :SUB], 1, 1))
        if n > SUB:
            ym = jnp.concatenate([ym, load(7, n - SUB)], axis=1)
    else:
        ym = load(lo - 1, n)
    if lo + n == total:
        yp = jnp.where(sub == last_row, -v[:, n - SUB :], pltpu.roll(v[:, n - SUB :], 7, 1))
        if n > SUB:
            yp = jnp.concatenate([load(lo + 1, n - SUB), yp], axis=1)
    else:
        yp = load(lo + 1, n)
    return ym + yp


def _blocks(total, size):
    return [(lo, min(size, total - lo)) for lo in range(0, total, size)]


def _planes0(src, f, z, u, emit, resid):
    total = src.shape[2]
    at, down, up = pl.ds(z, u), pl.ds(z - 1, u), pl.ds(z + 1, u)
    for lo, n in _blocks(total, BLOCK0):
        lane = _iota((u, n, LANES), -1)
        ends = (lane == 0, lane == 127)
        if resid:
            coef = tuple(jnp.where(e, 7.0, 6.0) for e in ends)
        else:
            coef = tuple(jnp.where(e, 2.0 * NINTH, 3.0 * NINTH) for e in ends)
        rows = pl.ds(lo, n)
        v = (src[0, at, rows, :], src[1, at, rows, :])
        x = (
            v[1] + jnp.where(ends[0], 0.0, pltpu.roll(v[1], 1, 2)),
            v[0] + jnp.where(ends[1], 0.0, pltpu.roll(v[0], 127, 2)),
        )
        for p in range(2):
            ys = _ysum(lambda r, m: src[p, at, pl.ds(r, m), :], lo, n, total, v[p])
            zs = src[p, down, rows, :] + src[p, up, rows, :]
            s = (x[p] + ys) + zs
            d = NINTH * (s - coef[p] * v[p]) if resid else coef[p] * v[p] + NINTH * s
            emit(p, lo, n, d + f[p, at, rows, :])


def _sweep0(src, dst, f, depth, n):
    lo, count = H - depth, n + 2 * depth
    step = min((SUB, 7, 6), key=lambda u: -(-count // u) * u)
    whole = -(-count // step) * step
    lo -= (whole - count) // 2

    def body(z):
        def emit(p, row, m, value):
            dst[p, pl.ds(z, step), pl.ds(row, m), :] = value

        _planes0(src, f, z, step, emit, False)

    _loop(lo, whole, step, body)


def _pairs(value):
    value = value.reshape(value.shape[0] // 2, 2, *value.shape[1:])
    return value[:, 0] + value[:, 1]


def _restrict0(src, f, coarse, tmp, yh, n):
    half = (src.shape[2] - SUB) // 2
    step = 4

    def body(zc):
        acc = {}

        def emit(p, lo, m, value):
            acc[lo] = (acc[lo][0] + value, m) if lo in acc else (value, m)

        _planes0(src, f, H + 2 * zc, 2 * step, emit, True)
        for lo, (value, m) in acc.items():
            tmp[pl.ds(0, step), pl.ds(lo, m), :] = _pairs(value)
        even = tmp[pl.ds(0, step), pl.ds(SUB * yh, half, stride=2), :]
        odd = tmp[pl.ds(0, step), pl.ds(SUB * yh + 1, half, stride=2), :]
        coarse[pl.ds(H + zc, step), pl.ds(pl.multiple_of(SUB * yh, SUB), half), :] = 0.5 * (even + odd)

    _loop(0, n // 2, step, body)


def _prolong_zy(coarse, zc, u, start, n, at_top, at_end, last_row=7):
    sub = _iota((2 * u, SUB, LANES), -2)

    def load(r, m):
        rows = pl.ds(r, m)
        c = NEAR * coarse[pl.ds(zc, u), rows, :]
        low = c + FAR * coarse[pl.ds(zc - 1, u), rows, :]
        high = c + FAR * coarse[pl.ds(zc + 1, u), rows, :]
        return jnp.stack([low, high], axis=1).reshape(2 * u, m, LANES)

    c = load(start, n)
    if at_top:
        cm = jnp.where(sub == 0, -c[:, :SUB], pltpu.roll(c[:, :SUB], 1, 1))
        if n > SUB:
            cm = jnp.concatenate([cm, load(start + 7, n - SUB)], axis=1)
    else:
        cm = load(start - 1, n)
    if at_end:
        cp = jnp.where(sub == last_row, -c[:, n - SUB :], pltpu.roll(c[:, n - SUB :], 7, 1))
        if n > SUB:
            cp = jnp.concatenate([load(start + 1, n - SUB), cp], axis=1)
    else:
        cp = load(start + 1, n)
    return NEAR * c + FAR * cm, NEAR * c + FAR * cp


def _y_parts(rows, offset, block):
    parts = []
    whole = rows // 16 * SUB
    for lo, n in _blocks(whole, block):
        end = lo + n == whole and rows % 16 == 0
        parts.append((offset + lo, n, 2 * lo, 2 * n, lo == 0, end, 0))
    if rows % 16:
        if rows == SUB:
            parts.append((offset, SUB, 0, SUB, True, True, 0))
        else:
            parts.append((offset + whole - 4, SUB, rows - SUB, SUB, False, True, SUB))
    return parts


def _prolong0(coarse, u, tmp, yh, depth, n):
    parts = _y_parts(u.shape[2], 4 * yh, BLOCKP)
    step = 2
    around = (depth + 1) // 2

    def body(zc):
        fine_at = pl.ds(H + 2 * (zc - H), 2 * step)
        for start, m, fine, count, top, end, skip in parts:
            pair = _prolong_zy(coarse, zc, step, start, m, top, end)
            lane = _iota((2 * step, m, LANES), -1)
            for parity in range(2):
                edge = lane == (0 if parity == 0 else 127)
                slots = pl.ds(2 * step * parity, 2 * step)
                for yc, c in enumerate(pair):
                    side = jnp.where(edge, -c, pltpu.roll(c, 1 if parity == 0 else 127, 2))
                    tmp[slots, pl.ds(fine - skip + yc, m, stride=2), :] = NEAR * c + FAR * side
                u[parity, fine_at, pl.ds(fine, count), :] += tmp[slots, pl.ds(fine, count), :]

    _loop(H - around, n // 2 + 2 * around, step, body)


def _planes(src, b, z, u, stride, emit, resid):
    total = src.shape[1]
    at = pl.ds(z, u)
    for lo, n in _blocks(total, BLOCK1):
        lane = _iota((u, n, LANES), -1)
        first, last = lane < stride, lane >= LANES - stride
        edge = jnp.where(first, 1.0, 0.0) + jnp.where(last, 1.0, 0.0)
        coef = 6.0 + edge if resid else (3.0 - edge) * NINTH
        rows = pl.ds(lo, n)
        v = src[at, rows, :]
        x = jnp.where(first, 0.0, pltpu.roll(v, stride, 2)) + jnp.where(last, 0.0, pltpu.roll(v, LANES - stride, 2))
        ys = _ysum(lambda r, m: src[at, pl.ds(r, m), :], lo, n, total, v)
        s = (x + ys) + (src[pl.ds(z - 1, u), rows, :] + src[pl.ds(z + 1, u), rows, :])
        d = NINTH * (s - coef * v) if resid else coef * v + NINTH * s
        emit(lo, n, d + b[at, rows, :])


def _sweep(src, dst, b, stride, lo, count):
    tiles = src.shape[1] // SUB
    step = max(u for u in range(1, count + 1) if count % u == 0 and u * tiles <= VREGS)

    def body(z):
        def emit(row, m, value):
            dst[pl.ds(z, step), pl.ds(row, m), :] = value

        _planes(src, b, z, step, stride, emit, False)

    _loop(lo, count, step, body)


def _restrict(src, b, stride, tmp, fine_lo, coarse, coarse_lo, count, fine_row, coarse_row, rows, step):
    def body(i):
        acc = {}

        def emit(lo, m, value):
            acc[lo] = (value, m)

        _planes(src, b, fine_lo + 2 * i, 2 * step, stride, emit, True)
        slots = pl.ds(0, step)
        for lo, (value, m) in acc.items():
            tmp[slots, pl.ds(lo, m), :] = _pairs(value)
        s = tmp[slots, pl.ds(fine_row, rows, stride=2), :] + tmp[slots, pl.ds(fine_row + 1, rows, stride=2), :]
        s = 0.5 * (s + pltpu.roll(s, LANES - stride, 2))
        row = coarse_row if isinstance(coarse_row, int) else pl.multiple_of(coarse_row, SUB)
        coarse[pl.ds(coarse_lo + i, step), pl.ds(row, rows), :] = s

    _loop(0, count, step, body)


def _prolong(coarse, v, stride, tmp, fine_lo, coarse_lo, count, offset, step, last_row=7):
    parts = _y_parts(v.shape[1], offset, BLOCKP)

    def body(i):
        fine_at = pl.ds(fine_lo + 2 * i, 2 * step)
        slots = pl.ds(0, 2 * step)
        for start, m, fine, n, top, end, skip in parts:
            lane = _iota((2 * step, m, LANES), -1)
            is_high = jnp.bitwise_and(lane, stride) != 0
            edge = (is_high & (lane >= LANES - 2 * stride)) | (jnp.logical_not(is_high) & (lane < 2 * stride))
            for yc, c in enumerate(_prolong_zy(coarse, coarse_lo + i, step, start, m, top, end, last_row)):
                own = jnp.where(is_high, pltpu.roll(c, stride, 2), c)
                side = jnp.where(is_high, pltpu.roll(c, LANES - stride, 2), pltpu.roll(c, 2 * stride, 2))
                side = jnp.where(edge, -own, side)
                tmp[slots, pl.ds(fine - skip + yc, m, stride=2), :] = NEAR * own + FAR * side
            v[fine_at, pl.ds(fine, n), :] += tmp[slots, pl.ds(fine, n), :]

    _loop(0, count, step, body)


def _mirror(ref, planes, ghost):
    def fill(k, carry=0):
        ref[ghost - 1 - k] = -ref[ghost + k]
        ref[ghost + planes + k] = -ref[ghost + planes - 1 - k]
        return carry

    if ghost == 1:
        fill(0)
    else:
        lax.fori_loop(0, ghost, fill, 0)


def _split_dot(x, m, left=False):
    hi = x.astype(jnp.bfloat16).astype(F32)
    rest = x - hi
    mid = rest.astype(jnp.bfloat16).astype(F32)
    low = rest - mid
    dot = functools.partial(jnp.dot, preferred_element_type=F32)
    if left:
        return (dot(m, hi) + dot(m, mid)) + dot(m, low)
    return (dot(hi, m) + dot(mid, m)) + dot(low, m)


def _kernel(u_in, f_in, inv, out, u0, u1, f, b1, v1a, v1b, b2, v2a, v2b, b3, v3a, v3b, b4, v4a, v4b, b5, v5a, v5b,
            b6, v6, tmp, send, recv, local):
    gz, gy, gx = (lax.axis_index(name) for name in ("gz", "gy", "gx"))
    zq, yh = 2 * gz + gx, gy
    core0, rows0 = u0.shape[1] - 2 * H, u0.shape[2] - SUB
    n1, n2, n3 = core0 // 2, core0 // 4, core0 // SUB
    r1, r2, r3 = rows0 // 2, rows0 // 4, rows0 // SUB
    counter = [0]

    def to(z, y, x):
        return {"gz": z, "gy": y, "gx": x}

    def remote(src, dst, slot, device):
        return pltpu.make_async_remote_copy(src_ref=src, dst_ref=dst, send_sem=send.at[slot], recv_sem=recv.at[slot],
                                            device_id=device, device_id_type=MESH)

    def new_slot():
        counter[0] += 1
        return counter[0] - 1

    barrier = pltpu.get_barrier_semaphore()
    others = [(a, b, c) for a in range(2) for b in range(2) for c in range(2) if a + b + c]
    for a, b, c in others:
        pl.semaphore_signal(barrier, inc=1, device_id=to(lax.rem(gz + a, 2), lax.rem(gy + b, 2), lax.rem(gx + c, 2)),
                            device_id_type=MESH)
    pl.semaphore_wait(barrier, len(others))

    def scatter(brick, window, d, lsem):
        waits = []
        n = core0 + d

        def mine(t):
            return brick.at[pl.ds(t * (core0 - d), n)]

        def place(half, t, row, count):
            return window.at[half, pl.ds(H - t * d, n), pl.ds(row, count)]

        row_src = pl.multiple_of((1 - gy) * (rows0 - SUB), SUB)
        row_dst = pl.multiple_of(gy * rows0, SUB)
        row_in = pl.multiple_of((1 - gy) * rows0, SUB)
        core_row = pl.multiple_of(SUB * gy, SUB)
        own = pltpu.make_async_copy(mine(gx), place(gx, gx, core_row, rows0), local.at[lsem])
        own.start()
        waits.append(own.wait)
        t_far = 1 - gz
        z_src = (1 - gz) * (LANES - d)
        z_dst = jnp.where(gz == 0, H - d, H + core0)
        z_in = jnp.where(gz == 0, H + core0, H - d)
        inner = gx == 1 - gz
        slots = {(kind, s): new_slot() for kind in ("z", "d") for s in range(2)}
        for s in range(2):
            cz = remote(brick.at[pl.ds(z_src, d)], window.at[s, pl.ds(z_dst, d), pl.ds(core_row, rows0)],
                        slots["z", s], to(1 - gz, gy, 1 - t_far))
            cd = remote(brick.at[pl.ds(z_src, d), pl.ds(row_src, SUB)], window.at[s, pl.ds(z_dst, d), pl.ds(row_dst, SUB)],
                        slots["d", s], to(1 - gz, 1 - gy, 1 - t_far))
            rz = remote(brick.at[pl.ds(z_src, d)], window.at[s, pl.ds(z_in, d), pl.ds(core_row, rows0)],
                        slots["z", s], to(1 - gz, gy, 1 - t_far))
            rd = remote(brick.at[pl.ds(z_src, d), pl.ds(row_src, SUB)], window.at[s, pl.ds(z_in, d), pl.ds(row_in, SUB)],
                        slots["d", s], to(1 - gz, 1 - gy, 1 - t_far))

            @pl.when(gx == s)
            def _():
                cz.start()
                cd.start()

            def wait(cz=cz, cd=cd, rz=rz, rd=rd, s=s):
                @pl.when(gx == s)
                def _():
                    cz.wait_send()
                    cd.wait_send()

                @pl.when(inner)
                def _():
                    rz.wait_recv()
                    rd.wait_recv()

            waits.append(wait)
        slots = {(s, t): new_slot() for s in range(2) for t in range(2)}
        for s in range(2):
            for t in range(2):
                cy = remote(brick.at[pl.ds(t * (core0 - d), n), pl.ds(row_src, SUB)], place(s, t, row_dst, SUB),
                            slots[s, t], to(gz, 1 - gy, t))
                ry = remote(brick.at[pl.ds(t * (core0 - d), n), pl.ds(row_src, SUB)], place(s, t, row_in, SUB),
                            slots[s, t], to(gz, 1 - gy, t))

                @pl.when(gx == s)
                def _():
                    cy.start()

                def wait(cy=cy, ry=ry, s=s, t=t):
                    @pl.when(gx == s)
                    def _():
                        cy.wait_send()

                    @pl.when(gx == t)
                    def _():
                        ry.wait_recv()

                waits.append(wait)
        slot = new_slot()
        cp = remote(mine(1 - gx), place(gx, 1 - gx, core_row, rows0), slot, to(gz, gy, 1 - gx))
        rp = remote(mine(gx), place(1 - gx, gx, core_row, rows0), slot, to(gz, gy, 1 - gx))
        cp.start()

        def wait():
            cp.wait_send()
            rp.wait_recv()

        waits.append(wait)
        return waits

    def reflect(ref, n, d, lead):
        def fill(dst, src):
            def step(k, carry):
                for p in range(lead):
                    r = ref.at[p] if lead > 1 else ref
                    r[dst(k)] = -r[src(k)]
                return carry

            lax.fori_loop(0, d, step, 0)

        @pl.when(zq == 0)
        def _():
            fill(lambda k: H - 1 - k, lambda k: H + k)

        @pl.when(zq == 3)
        def _():
            fill(lambda k: H + n + k, lambda k: H + n - 1 - k)

    def exchange(ref, n, m, d, lead):
        pre = (slice(None),) if lead > 1 else ()

        def at(z, dz, row, dr):
            return ref.at[pre + (pl.ds(z, dz), pl.ds(pl.multiple_of(row, SUB), dr))]

        core_row = SUB * yh
        row_src = (1 - yh) * (m - SUB) + yh * SUB
        row_dst = yh * m
        row_in = (1 - yh) * m
        waits = []
        slot = new_slot()
        across = remote(at(H, n, row_src, SUB), at(H, n, row_dst, SUB), slot, to(gz, 1 - gy, gx))
        arrive = remote(at(H, n, row_src, SUB), at(H, n, row_in, SUB), slot, to(gz, 1 - gy, gx))
        jobs = []
        for up in (False, True):
            qz = jnp.minimum(gz + gx, 1) if up else jnp.maximum(gz + gx - 1, 0)
            qx = 1 - gx
            z_src = H + n - d if up else H
            z_dst = H - d if up else H + n
            z_in = H - d if up else H + n
            sends = zq < 3 if up else zq > 0
            takes = zq > 0 if up else zq < 3
            sz, sd = new_slot(), new_slot()
            cz = remote(at(z_src, d, core_row, m), at(z_dst, d, core_row, m), sz, to(qz, gy, qx))
            cd = remote(at(z_src, d, row_src, SUB), at(z_dst, d, row_dst, SUB), sd, to(qz, 1 - gy, qx))
            rz = remote(at(z_src, d, core_row, m), at(z_in, d, core_row, m), sz, to(qz, gy, qx))
            rd = remote(at(z_src, d, row_src, SUB), at(z_in, d, row_in, SUB), sd, to(qz, 1 - gy, qx))
            jobs.append((sends, takes, cz, cd, rz, rd))
        for sends, _, cz, cd, _, _ in jobs:

            @pl.when(sends)
            def _():
                cd.start()
                cz.start()

        across.start()

        def wait():
            across.wait_send()
            arrive.wait_recv()
            for sends, takes, cz, cd, rz, rd in jobs:

                @pl.when(sends)
                def _():
                    cz.wait_send()
                    cd.wait_send()

                @pl.when(takes)
                def _():
                    rz.wait_recv()
                    rd.wait_recv()

        waits.append(wait)
        return wait

    waits_u = scatter(u_in, u0, DU, 0)
    waits_f = scatter(f_in, f, DF, 1)

    col = lax.broadcasted_iota(jnp.int32, (256, 256), 1)
    row = lax.broadcasted_iota(jnp.int32, (256, 256), 0)
    split = (row == 2 * jnp.bitwise_and(col, 127) + lax.shift_right_logical(col, 7)).astype(F32)
    merge = (col == 2 * jnp.bitwise_and(row, 127) + lax.shift_right_logical(row, 7)).astype(F32)
    def lanes(shape, axis, sign):
        cell = lax.broadcasted_iota(jnp.int32, shape, 1 - axis)
        spot = lax.broadcasted_iota(jnp.int32, shape, axis)
        z = lax.shift_right_logical(cell, 4)
        y = jnp.bitwise_and(lax.shift_right_logical(cell, 2), 3)
        x = jnp.bitwise_and(cell, 3)
        return (spot == jnp.bitwise_and(32 * x + sign * (4 * z + y), 127)).astype(F32)

    table = _split_dot(_split_dot(inv[...], lanes((64, LANES), 1, -1)), lanes((LANES, 64), 0, 1), left=True) * (9.0 * 16.0)

    for wait in waits_u:
        wait()

    def permute(ref, m, scale, lo, count, dst):
        def body(z):
            for k in range(2):
                x = jnp.concatenate([ref[0, z + k], ref[1, z + k]], axis=1)
                y = _split_dot(x, m)
                if scale is not None:
                    y = y * scale
                dst[0, z + k] = y[:, :LANES]
                dst[1, z + k] = y[:, LANES:]

        _loop(lo, count, 2, body)

    reflect(u0, core0, DU, 2)
    permute(u0, split, None, H - DU, core0 + 2 * DU, u0)
    for wait in waits_f:
        wait()
    reflect(f, core0, DF, 2)
    permute(f, split, NINTH / 65536.0, H - DF, core0 + 2 * DF, f)

    def bottom():
        lane, sub = _iota(v6.shape[1:], -1), _iota(v6.shape[1:], -2)
        valid = jnp.bitwise_and(lane, 31) == 0
        total = jnp.zeros(v6.shape[1:], F32)
        for i in range(COARSE * COARSE):
            z, y = divmod(i, COARSE)
            total = total + pltpu.roll(jnp.where(valid & (sub == y), b6[z], 0.0), i, 1)
        for shift in (4, 2, 1):
            total = total + pltpu.roll(total, shift, 0)
        e6 = jnp.dot(total, table, precision=lax.Precision.HIGHEST, preferred_element_type=F32)
        for z in range(COARSE):
            plane = e6
            for y in range(COARSE):
                plane = jnp.where(sub == y, pltpu.roll(e6, COARSE * z + y, 1), plane)
            v6[1 + z] = plane
        _mirror(v6, COARSE, 1)

    for cycle in range(CYCLES):
        c1, c2, c3 = b1.at[cycle], b2.at[cycle], b3.at[cycle]
        more = cycle + 1 < CYCLES
        if cycle == 0:
            _sweep0(u0, u1, f, 2, core0)
            _sweep0(u1, u0, f, 1, core0)
        _restrict0(u0, f, c1, tmp, yh, core0)
        wait_b1 = exchange(c1, n1, r1, H, 1)
        wait_b1()
        reflect(c1, n1, H, 1)
        _sweep(c1, v1a, c1, 1, 1, c1.shape[0] - 2)
        _restrict(v1a, c1, 1, tmp, H, c2, H, n2, SUB * yh, SUB * yh, r2, 4)
        wait_b2 = exchange(c2, n2, r2, H, 1)
        wait_b2()
        reflect(c2, n2, H, 1)
        _sweep(c2, v2a, c2, 2, 1, c2.shape[0] - 2)
        _restrict(v2a, c2, 2, tmp, H, c3, G3 + n3 * zq, n3, SUB * yh, r3 * yh, r3, 4)
        waits3 = []

        def block(z, y, x):
            return c3.at[pl.ds(G3 + n3 * (2 * z + x), n3), pl.ds(pl.multiple_of(r3 * y, SUB), r3)]

        for a, b, c in others:
            z, y, x = lax.rem(gz + a, 2), lax.rem(gy + b, 2), lax.rem(gx + c, 2)
            slot = new_slot()
            src = block(gz, gy, gx)
            give = remote(src, src, slot, to(z, y, x))
            take = remote(src, block(z, y, x), slot, to(z, y, x))
            give.start()
            waits3.append((give, take))
        for give, take in waits3:
            give.wait_send()
            take.wait_recv()
        depth = DV if more else 2
        wait_v = exchange(u0, core0, rows0, depth, 2)
        small = ((4, G3, c3, v3a, v3b), (SUB, 1, b4, v4a, v4b), (16, 1, b5, v5a, v5b))
        after = ((b4, 1), (b5, 1), (b6, 0))
        for (stride, g, b, va, vb), (coarse, ghost) in zip(small, after):
            n = b.shape[0] - 2 * g
            _mirror(b, n, g)
            _sweep(b, va, b, stride, g, n)
            _mirror(va, n, g)
            _restrict(va, b, stride, tmp, g, coarse, ghost, n // 2, 0, 0, coarse.shape[1], 4)
        bottom()
        coarse, last_row = v6, COARSE - 1
        for stride, g, b, va, vb in reversed(small):
            n = b.shape[0] - 2 * g
            _prolong(coarse, va, stride, tmp, g, 1, n // 2, 0, 4, last_row)
            _mirror(va, n, g)
            _sweep(va, vb, b, stride, g, n)
            _mirror(vb, n, g)
            _sweep(vb, va, b, stride, g, n)
            _mirror(va, n, g)
            coarse, last_row = va, SUB - 1
        half = H // 2
        _prolong(v3a, v2a, 2, tmp, 0, G3 + n3 * zq - half, n3 + H, (r3 - 4) * yh, 2)
        _sweep(v2a, v2b, c2, 2, 2, c2.shape[0] - 4)
        _sweep(v2b, v2a, c2, 2, 2, c2.shape[0] - 4)
        _prolong(v2a, v1a, 1, tmp, 0, half, n2 + H, 4 * yh, 2)
        _sweep(v1a, v1b, c1, 1, 2, c1.shape[0] - 4)
        _sweep(v1b, v1a, c1, 1, 2, c1.shape[0] - 4)
        wait_v()
        reflect(u0, core0, depth, 2)
        _prolong0(v1a, u0, tmp, yh, depth, core0)
        for left in reversed(range(0, depth - 1 if more else depth, 2)):
            _sweep0(u0, u1, f, left + 1 + more, core0)
            _sweep0(u1, u0, f, left + more, core0)

    permute(u0, merge, None, H, core0, u1)
    core_row = pl.multiple_of(SUB * yh, SUB)

    def part(half):
        return u1.at[half, pl.ds(H, core0), pl.ds(core_row, rows0)]

    slot = new_slot()
    keep = pltpu.make_async_copy(part(gx), out.at[pl.ds(core0 * gx, core0)], local.at[2])
    give = remote(part(1 - gx), out.at[pl.ds(core0 * gx, core0)], slot, to(gz, gy, 1 - gx))
    take = remote(part(1 - gx), out.at[pl.ds(core0 * (1 - gx), core0)], slot, to(gz, gy, 1 - gx))
    give.start()
    keep.start()
    keep.wait()
    give.wait_send()
    take.wait_recv()


SLOTS = 80


def solution(mesh):
    spec = P(("batch", "gz"), "gy", "gx")

    def local(rhs, init, inv):
        def vm(*shape):
            return pltpu.VMEM(shape, F32)

        def level(planes, rows, *lead):
            return [vm(*lead, planes, rows, LANES), vm(planes, rows, LANES), vm(planes, rows, LANES)]

        nz, ny = init.shape[0] // 2, init.shape[1]
        scratch = [vm(2, nz + 2 * H, ny + SUB, LANES)] * 3
        for l in (1, 2):
            scratch += level((nz >> l) + 2 * H, (ny >> l) + SUB, CYCLES)
        scratch += level(nz // 2 + 2 * G3, nz // 2, CYCLES)
        scratch += level(nz // 4 + 2, nz // 4) + level(nz // SUB + 2, SUB)
        scratch += [vm(COARSE, SUB, LANES), vm(COARSE + 2, SUB, LANES), vm(16, ny + 3 * SUB, LANES)]
        sems = pltpu.SemaphoreType.DMA((SLOTS,))
        call = pl.pallas_call(
            _kernel,
            out_shape=jax.ShapeDtypeStruct(init.shape, F32),
            in_specs=[pl.BlockSpec(memory_space=pl.ANY)] * 2 + [pl.BlockSpec(memory_space=pltpu.VMEM)],
            out_specs=pl.BlockSpec(memory_space=pl.ANY),
            scratch_shapes=scratch + [sems] * 3,
            compiler_params=pltpu.CompilerParams(
                collective_id=0, has_side_effects=True, vmem_limit_bytes=62 * 2**20
            ),
            name="vcycles",
        )
        return call(init, rhs, inv)

    return jax.shard_map(local, mesh=mesh, in_specs=(spec, spec, P()), out_specs=spec, check_vma=False)
```

```python
import functools

import jax
import jax.numpy as jnp
from jax import lax
from jax.experimental import pallas as pl
from jax.experimental.pallas import tpu as pltpu
from jax.sharding import PartitionSpec as P

MESH = pl.DeviceIdType.MESH
F32 = jnp.float32
NINTH = 1.0 / 9.0
H = 6
G3 = 4
CYCLES = 2
DU, DF, DV = 3, 4, 5
SUB, LANES = 8, 128
NEAR, FAR = 0.75, 0.25
COARSE = 4
VREGS = 72
PERMUTE = 8
BLOCK0 = 136
BLOCK1 = 136
BLOCKP = 64


def _loop(lo, count, step, body):
    assert count % step == 0

    def run(i, carry):
        body(lo + i * step)
        return carry

    if count == step:
        body(lo)
    else:
        lax.fori_loop(0, count // step, run, 0)


def _iota(shape, axis):
    return lax.broadcasted_iota(jnp.int32, shape, len(shape) + axis)


def _ysum(load, lo, n, total, v, last_row=7):
    sub = _iota((v.shape[0], SUB, LANES), -2)
    if lo == 0:
        ym = jnp.where(sub == 0, -v[:, :SUB], pltpu.roll(v[:, :SUB], 1, 1))
        if n > SUB:
            ym = jnp.concatenate([ym, load(7, n - SUB)], axis=1)
    else:
        ym = load(lo - 1, n)
    if lo + n == total:
        yp = jnp.where(sub == last_row, -v[:, n - SUB :], pltpu.roll(v[:, n - SUB :], 7, 1))
        if n > SUB:
            yp = jnp.concatenate([load(lo + 1, n - SUB), yp], axis=1)
    else:
        yp = load(lo + 1, n)
    return ym + yp


def _blocks(total, size):
    return [(lo, min(size, total - lo)) for lo in range(0, total, size)]


def _planes0(src, f, z, u, emit, resid):
    total = src.shape[2]
    at, down, up = pl.ds(z, u), pl.ds(z - 1, u), pl.ds(z + 1, u)
    for lo, n in _blocks(total, BLOCK0):
        lane = _iota((u, n, LANES), -1)
        ends = (lane == 0, lane == 127)
        if resid:
            coef = tuple(jnp.where(e, 7.0, 6.0) for e in ends)
        else:
            coef = tuple(jnp.where(e, 2.0 * NINTH, 3.0 * NINTH) for e in ends)
        rows = pl.ds(lo, n)
        v = (src[0, at, rows, :], src[1, at, rows, :])
        x = (
            v[1] + jnp.where(ends[0], 0.0, pltpu.roll(v[1], 1, 2)),
            v[0] + jnp.where(ends[1], 0.0, pltpu.roll(v[0], 127, 2)),
        )
        for p in range(2):
            ys = _ysum(lambda r, m: src[p, at, pl.ds(r, m), :], lo, n, total, v[p])
            zs = src[p, down, rows, :] + src[p, up, rows, :]
            s = (x[p] + ys) + zs
            d = NINTH * (s - coef[p] * v[p]) if resid else coef[p] * v[p] + NINTH * s
            emit(p, lo, n, d + f[p, at, rows, :])


def _sweep0(src, dst, f, depth, n):
    lo, count = H - depth, n + 2 * depth
    step = min((SUB, 7, 6), key=lambda u: -(-count // u) * u)
    whole = -(-count // step) * step
    lo -= (whole - count) // 2

    def body(z):
        def emit(p, row, m, value):
            dst[p, pl.ds(z, step), pl.ds(row, m), :] = value

        _planes0(src, f, z, step, emit, False)

    _loop(lo, whole, step, body)


def _pairs(value):
    value = value.reshape(value.shape[0] // 2, 2, *value.shape[1:])
    return value[:, 0] + value[:, 1]


def _restrict0(src, f, coarse, tmp, yh, n):
    half = (src.shape[2] - SUB) // 2
    step = 4

    def body(zc):
        acc = {}

        def emit(p, lo, m, value):
            acc[lo] = (acc[lo][0] + value, m) if lo in acc else (value, m)

        _planes0(src, f, H + 2 * zc, 2 * step, emit, True)
        for lo, (value, m) in acc.items():
            tmp[pl.ds(0, step), pl.ds(lo, m), :] = _pairs(value)
        even = tmp[pl.ds(0, step), pl.ds(SUB * yh, half, stride=2), :]
        odd = tmp[pl.ds(0, step), pl.ds(SUB * yh + 1, half, stride=2), :]
        coarse[pl.ds(H + zc, step), pl.ds(pl.multiple_of(SUB * yh, SUB), half), :] = 0.5 * (even + odd)

    _loop(0, n // 2, step, body)


def _prolong_zy(coarse, zc, u, start, n, at_top, at_end, last_row=7):
    sub = _iota((2 * u, SUB, LANES), -2)

    def load(r, m):
        rows = pl.ds(r, m)
        c = NEAR * coarse[pl.ds(zc, u), rows, :]
        low = c + FAR * coarse[pl.ds(zc - 1, u), rows, :]
        high = c + FAR * coarse[pl.ds(zc + 1, u), rows, :]
        return jnp.stack([low, high], axis=1).reshape(2 * u, m, LANES)

    c = load(start, n)
    if at_top:
        cm = jnp.where(sub == 0, -c[:, :SUB], pltpu.roll(c[:, :SUB], 1, 1))
        if n > SUB:
            cm = jnp.concatenate([cm, load(start + 7, n - SUB)], axis=1)
    else:
        cm = load(start - 1, n)
    if at_end:
        cp = jnp.where(sub == last_row, -c[:, n - SUB :], pltpu.roll(c[:, n - SUB :], 7, 1))
        if n > SUB:
            cp = jnp.concatenate([load(start + 1, n - SUB), cp], axis=1)
    else:
        cp = load(start + 1, n)
    return NEAR * c + FAR * cm, NEAR * c + FAR * cp


def _y_parts(rows, offset, block):
    parts = []
    whole = rows // 16 * SUB
    for lo, n in _blocks(whole, block):
        end = lo + n == whole and rows % 16 == 0
        parts.append((offset + lo, n, 2 * lo, 2 * n, lo == 0, end, 0))
    if rows % 16:
        if rows == SUB:
            parts.append((offset, SUB, 0, SUB, True, True, 0))
        else:
            parts.append((offset + whole - 4, SUB, rows - SUB, SUB, False, True, SUB))
    return parts


def _prolong0(coarse, u, tmp, yh, depth, n):
    parts = _y_parts(u.shape[2], 4 * yh, BLOCKP)
    step = 2
    around = (depth + 1) // 2

    def body(zc):
        fine_at = pl.ds(H + 2 * (zc - H), 2 * step)
        for start, m, fine, count, top, end, skip in parts:
            pair = _prolong_zy(coarse, zc, step, start, m, top, end)
            lane = _iota((2 * step, m, LANES), -1)
            for parity in range(2):
                edge = lane == (0 if parity == 0 else 127)
                slots = pl.ds(2 * step * parity, 2 * step)
                for yc, c in enumerate(pair):
                    side = jnp.where(edge, -c, pltpu.roll(c, 1 if parity == 0 else 127, 2))
                    tmp[slots, pl.ds(fine - skip + yc, m, stride=2), :] = NEAR * c + FAR * side
                u[parity, fine_at, pl.ds(fine, count), :] += tmp[slots, pl.ds(fine, count), :]

    _loop(H - around, n // 2 + 2 * around, step, body)


def _planes(src, b, z, u, stride, emit, resid):
    total = src.shape[1]
    at = pl.ds(z, u)
    for lo, n in _blocks(total, BLOCK1):
        lane = _iota((u, n, LANES), -1)
        first, last = lane < stride, lane >= LANES - stride
        edge = jnp.where(first, 1.0, 0.0) + jnp.where(last, 1.0, 0.0)
        coef = 6.0 + edge if resid else (3.0 - edge) * NINTH
        rows = pl.ds(lo, n)
        v = src[at, rows, :]
        x = jnp.where(first, 0.0, pltpu.roll(v, stride, 2)) + jnp.where(last, 0.0, pltpu.roll(v, LANES - stride, 2))
        ys = _ysum(lambda r, m: src[at, pl.ds(r, m), :], lo, n, total, v)
        s = (x + ys) + (src[pl.ds(z - 1, u), rows, :] + src[pl.ds(z + 1, u), rows, :])
        d = NINTH * (s - coef * v) if resid else coef * v + NINTH * s
        emit(lo, n, d + b[at, rows, :])


def _sweep(src, dst, b, stride, lo, count):
    tiles = src.shape[1] // SUB
    step = max(u for u in range(1, count + 1) if count % u == 0 and u * tiles <= VREGS)

    def body(z):
        def emit(row, m, value):
            dst[pl.ds(z, step), pl.ds(row, m), :] = value

        _planes(src, b, z, step, stride, emit, False)

    _loop(lo, count, step, body)


def _restrict(src, b, stride, tmp, fine_lo, coarse, coarse_lo, count, fine_row, coarse_row, rows, step):
    def body(i):
        acc = {}

        def emit(lo, m, value):
            acc[lo] = (value, m)

        _planes(src, b, fine_lo + 2 * i, 2 * step, stride, emit, True)
        slots = pl.ds(0, step)
        for lo, (value, m) in acc.items():
            tmp[slots, pl.ds(lo, m), :] = _pairs(value)
        s = tmp[slots, pl.ds(fine_row, rows, stride=2), :] + tmp[slots, pl.ds(fine_row + 1, rows, stride=2), :]
        s = 0.5 * (s + pltpu.roll(s, LANES - stride, 2))
        row = coarse_row if isinstance(coarse_row, int) else pl.multiple_of(coarse_row, SUB)
        coarse[pl.ds(coarse_lo + i, step), pl.ds(row, rows), :] = s

    _loop(0, count, step, body)


def _prolong(coarse, v, stride, tmp, fine_lo, coarse_lo, count, offset, step, last_row=7):
    parts = _y_parts(v.shape[1], offset, BLOCKP)

    def body(i):
        fine_at = pl.ds(fine_lo + 2 * i, 2 * step)
        slots = pl.ds(0, 2 * step)
        for start, m, fine, n, top, end, skip in parts:
            lane = _iota((2 * step, m, LANES), -1)
            is_high = jnp.bitwise_and(lane, stride) != 0
            edge = (is_high & (lane >= LANES - 2 * stride)) | (jnp.logical_not(is_high) & (lane < 2 * stride))
            for yc, c in enumerate(_prolong_zy(coarse, coarse_lo + i, step, start, m, top, end, last_row)):
                own = jnp.where(is_high, pltpu.roll(c, stride, 2), c)
                side = jnp.where(is_high, pltpu.roll(c, LANES - stride, 2), pltpu.roll(c, 2 * stride, 2))
                side = jnp.where(edge, -own, side)
                tmp[slots, pl.ds(fine - skip + yc, m, stride=2), :] = NEAR * own + FAR * side
            v[fine_at, pl.ds(fine, n), :] += tmp[slots, pl.ds(fine, n), :]

    _loop(0, count, step, body)


def _mirror(ref, planes, ghost):
    def fill(k, carry=0):
        ref[ghost - 1 - k] = -ref[ghost + k]
        ref[ghost + planes + k] = -ref[ghost + planes - 1 - k]
        return carry

    if ghost == 1:
        fill(0)
    else:
        lax.fori_loop(0, ghost, fill, 0)


def _split_dot(x, m, left=False):
    hi = x.astype(jnp.bfloat16).astype(F32)
    rest = x - hi
    mid = rest.astype(jnp.bfloat16).astype(F32)
    low = rest - mid
    dot = functools.partial(jnp.dot, preferred_element_type=F32)
    if left:
        return (dot(m, hi) + dot(m, mid)) + dot(m, low)
    return (dot(hi, m) + dot(mid, m)) + dot(low, m)


def _kernel(u_in, f_in, inv, out, u0, u1, f, b1, v1a, v1b, b2, v2a, v2b, b3, v3a, v3b, b4, v4a, v4b, b5, v5a, v5b,
            b6, v6, tmp, send, recv, local):
    gz, gy, gx = (lax.axis_index(name) for name in ("gz", "gy", "gx"))
    zq, yh = 2 * gz + gx, gy
    core0, rows0 = u0.shape[1] - 2 * H, u0.shape[2] - SUB
    n1, n2, n3 = core0 // 2, core0 // 4, core0 // SUB
    r1, r2, r3 = rows0 // 2, rows0 // 4, rows0 // SUB
    counter = [0]

    def to(z, y, x):
        return {"gz": z, "gy": y, "gx": x}

    def remote(src, dst, slot, device):
        return pltpu.make_async_remote_copy(src_ref=src, dst_ref=dst, send_sem=send.at[slot], recv_sem=recv.at[slot],
                                            device_id=device, device_id_type=MESH)

    def new_slot():
        counter[0] += 1
        return counter[0] - 1

    barrier = pltpu.get_barrier_semaphore()
    others = [(a, b, c) for a in range(2) for b in range(2) for c in range(2) if a + b + c]
    for a, b, c in others:
        pl.semaphore_signal(barrier, inc=1, device_id=to(lax.rem(gz + a, 2), lax.rem(gy + b, 2), lax.rem(gx + c, 2)),
                            device_id_type=MESH)
    pl.semaphore_wait(barrier, len(others))

    def seam(m, d, start):
        below = SUB - d
        return (1 - yh) * (m - d) + yh * start, (1 - yh) * below + yh * m, yh * below + (1 - yh) * m

    def scatter(brick, window, d, lsem):
        waits = []
        n = core0 + d

        def mine(t):
            return brick.at[pl.ds(t * (core0 - d), n)]

        def place(half, t, row, count):
            return window.at[half, pl.ds(H - t * d, n), pl.ds(row, count)]

        row_src, row_dst, row_in = seam(rows0, d, 0)
        core_row = pl.multiple_of(SUB * gy, SUB)
        own = pltpu.make_async_copy(mine(gx), place(gx, gx, core_row, rows0), local.at[lsem])
        own.start()
        waits.append(own.wait)
        t_far = 1 - gz
        z_src = (1 - gz) * (LANES - d)
        z_dst = jnp.where(gz == 0, H - d, H + core0)
        z_in = jnp.where(gz == 0, H + core0, H - d)
        inner = gx == 1 - gz
        slots = {(kind, s): new_slot() for kind in ("z", "d") for s in range(2)}
        for s in range(2):
            cz = remote(brick.at[pl.ds(z_src, d)], window.at[s, pl.ds(z_dst, d), pl.ds(core_row, rows0)],
                        slots["z", s], to(1 - gz, gy, 1 - t_far))
            cd = remote(brick.at[pl.ds(z_src, d), pl.ds(row_src, d)], window.at[s, pl.ds(z_dst, d), pl.ds(row_dst, d)],
                        slots["d", s], to(1 - gz, 1 - gy, 1 - t_far))
            rz = remote(brick.at[pl.ds(z_src, d)], window.at[s, pl.ds(z_in, d), pl.ds(core_row, rows0)],
                        slots["z", s], to(1 - gz, gy, 1 - t_far))
            rd = remote(brick.at[pl.ds(z_src, d), pl.ds(row_src, d)], window.at[s, pl.ds(z_in, d), pl.ds(row_in, d)],
                        slots["d", s], to(1 - gz, 1 - gy, 1 - t_far))

            @pl.when(gx == s)
            def _():
                cz.start()
                cd.start()

            def wait(cz=cz, cd=cd, rz=rz, rd=rd, s=s):
                @pl.when(gx == s)
                def _():
                    cz.wait_send()
                    cd.wait_send()

                @pl.when(inner)
                def _():
                    rz.wait_recv()
                    rd.wait_recv()

            waits.append(wait)
        slots = {(s, t): new_slot() for s in range(2) for t in range(2)}
        for s in range(2):
            for t in range(2):
                cy = remote(brick.at[pl.ds(t * (core0 - d), n), pl.ds(row_src, d)], place(s, t, row_dst, d),
                            slots[s, t], to(gz, 1 - gy, t))
                ry = remote(brick.at[pl.ds(t * (core0 - d), n), pl.ds(row_src, d)], place(s, t, row_in, d),
                            slots[s, t], to(gz, 1 - gy, t))

                @pl.when(gx == s)
                def _():
                    cy.start()

                def wait(cy=cy, ry=ry, s=s, t=t):
                    @pl.when(gx == s)
                    def _():
                        cy.wait_send()

                    @pl.when(gx == t)
                    def _():
                        ry.wait_recv()

                waits.append(wait)
        slot = new_slot()
        cp = remote(mine(1 - gx), place(gx, 1 - gx, core_row, rows0), slot, to(gz, gy, 1 - gx))
        rp = remote(mine(gx), place(1 - gx, gx, core_row, rows0), slot, to(gz, gy, 1 - gx))
        cp.start()

        def wait():
            cp.wait_send()
            rp.wait_recv()

        waits.append(wait)
        return waits

    def reflect(ref, n, d, lead):
        def fill(dst, src):
            def step(k, carry):
                for p in range(lead):
                    r = ref.at[p] if lead > 1 else ref
                    r[dst(k)] = -r[src(k)]
                return carry

            lax.fori_loop(0, d, step, 0)

        @pl.when(zq == 0)
        def _():
            fill(lambda k: H - 1 - k, lambda k: H + k)

        @pl.when(zq == 3)
        def _():
            fill(lambda k: H + n + k, lambda k: H + n - 1 - k)

    def exchange(ref, n, m, d, lead):
        pre = (slice(None),) if lead > 1 else ()

        def at(z, dz, row, dr):
            return ref.at[pre + (pl.ds(z, dz), pl.ds(row, dr))]

        core_row = pl.multiple_of(SUB * yh, SUB)
        row_src, row_dst, row_in = seam(m, d, SUB)
        waits = []
        slot = new_slot()
        across = remote(at(H, n, row_src, d), at(H, n, row_dst, d), slot, to(gz, 1 - gy, gx))
        arrive = remote(at(H, n, row_src, d), at(H, n, row_in, d), slot, to(gz, 1 - gy, gx))
        jobs = []
        for up in (False, True):
            qz = jnp.minimum(gz + gx, 1) if up else jnp.maximum(gz + gx - 1, 0)
            qx = 1 - gx
            z_src = H + n - d if up else H
            z_dst = H - d if up else H + n
            z_in = H - d if up else H + n
            sends = zq < 3 if up else zq > 0
            takes = zq > 0 if up else zq < 3
            sz, sd = new_slot(), new_slot()
            cz = remote(at(z_src, d, core_row, m), at(z_dst, d, core_row, m), sz, to(qz, gy, qx))
            cd = remote(at(z_src, d, row_src, d), at(z_dst, d, row_dst, d), sd, to(qz, 1 - gy, qx))
            rz = remote(at(z_src, d, core_row, m), at(z_in, d, core_row, m), sz, to(qz, gy, qx))
            rd = remote(at(z_src, d, row_src, d), at(z_in, d, row_in, d), sd, to(qz, 1 - gy, qx))
            jobs.append((sends, takes, cz, cd, rz, rd))
        for sends, _, cz, cd, _, _ in jobs:

            @pl.when(sends)
            def _():
                cd.start()
                cz.start()

        across.start()

        def wait():
            across.wait_send()
            arrive.wait_recv()
            for sends, takes, cz, cd, rz, rd in jobs:

                @pl.when(sends)
                def _():
                    cz.wait_send()
                    cd.wait_send()

                @pl.when(takes)
                def _():
                    rz.wait_recv()
                    rd.wait_recv()

        waits.append(wait)
        return wait

    waits_u = scatter(u_in, u0, DU, 0)
    waits_f = scatter(f_in, f, DF, 1)

    col = lax.broadcasted_iota(jnp.int32, (256, 256), 1)
    row = lax.broadcasted_iota(jnp.int32, (256, 256), 0)
    split = (row == 2 * jnp.bitwise_and(col, 127) + lax.shift_right_logical(col, 7)).astype(F32)
    merge = (col == 2 * jnp.bitwise_and(row, 127) + lax.shift_right_logical(row, 7)).astype(F32)
    def lanes(shape, axis, sign):
        cell = lax.broadcasted_iota(jnp.int32, shape, 1 - axis)
        spot = lax.broadcasted_iota(jnp.int32, shape, axis)
        z = lax.shift_right_logical(cell, 4)
        y = jnp.bitwise_and(lax.shift_right_logical(cell, 2), 3)
        x = jnp.bitwise_and(cell, 3)
        return (spot == jnp.bitwise_and(32 * x + sign * (4 * z + y), 127)).astype(F32)

    table = _split_dot(_split_dot(inv[...], lanes((64, LANES), 1, -1)), lanes((LANES, 64), 0, 1), left=True) * (9.0 * 16.0)

    for wait in waits_u:
        wait()

    def permute(ref, m, scale, lo, count, dst):
        step = max(u for u in range(1, PERMUTE + 1) if count % u == 0)

        def body(z):
            at = pl.ds(z, step)
            x = jnp.concatenate([ref[0, at], ref[1, at]], axis=-1)
            y = _split_dot(x.reshape(-1, 2 * LANES), m).reshape(x.shape)
            if scale is not None:
                y = y * scale
            dst[0, at] = y[..., :LANES]
            dst[1, at] = y[..., LANES:]

        _loop(lo, count, step, body)

    reflect(u0, core0, DU, 2)
    permute(u0, split, None, H - DU, core0 + 2 * DU, u0)
    for wait in waits_f:
        wait()
    reflect(f, core0, DF, 2)
    permute(f, split, NINTH / 65536.0, H - DF, core0 + 2 * DF, f)

    def bottom():
        lane, sub = _iota(v6.shape[1:], -1), _iota(v6.shape[1:], -2)
        valid = jnp.bitwise_and(lane, 31) == 0
        total = jnp.zeros(v6.shape[1:], F32)
        for i in range(COARSE * COARSE):
            z, y = divmod(i, COARSE)
            total = total + pltpu.roll(jnp.where(valid & (sub == y), b6[z], 0.0), i, 1)
        for shift in (4, 2, 1):
            total = total + pltpu.roll(total, shift, 0)
        e6 = jnp.dot(total, table, precision=lax.Precision.HIGHEST, preferred_element_type=F32)
        for z in range(COARSE):
            plane = e6
            for y in range(COARSE):
                plane = jnp.where(sub == y, pltpu.roll(e6, COARSE * z + y, 1), plane)
            v6[1 + z] = plane
        _mirror(v6, COARSE, 1)

    for cycle in range(CYCLES):
        c1, c2, c3 = b1.at[cycle], b2.at[cycle], b3.at[cycle]
        more = cycle + 1 < CYCLES
        if cycle == 0:
            _sweep0(u0, u1, f, 2, core0)
            _sweep0(u1, u0, f, 1, core0)
        _restrict0(u0, f, c1, tmp, yh, core0)
        wait_b1 = exchange(c1, n1, r1, H, 1)
        wait_b1()
        reflect(c1, n1, H, 1)
        _sweep(c1, v1a, c1, 1, 1, c1.shape[0] - 2)
        _restrict(v1a, c1, 1, tmp, H, c2, H, n2, SUB * yh, SUB * yh, r2, 4)
        wait_b2 = exchange(c2, n2, r2, H, 1)
        wait_b2()
        reflect(c2, n2, H, 1)
        _sweep(c2, v2a, c2, 2, 1, c2.shape[0] - 2)
        _restrict(v2a, c2, 2, tmp, H, c3, G3 + n3 * zq, n3, SUB * yh, r3 * yh, r3, 4)
        waits3 = []

        def block(z, y, x):
            return c3.at[pl.ds(G3 + n3 * (2 * z + x), n3), pl.ds(pl.multiple_of(r3 * y, SUB), r3)]

        for a, b, c in others:
            z, y, x = lax.rem(gz + a, 2), lax.rem(gy + b, 2), lax.rem(gx + c, 2)
            slot = new_slot()
            src = block(gz, gy, gx)
            give = remote(src, src, slot, to(z, y, x))
            take = remote(src, block(z, y, x), slot, to(z, y, x))
            give.start()
            waits3.append((give, take))
        for give, take in waits3:
            give.wait_send()
            take.wait_recv()
        depth = DV if more else 2
        wait_v = exchange(u0, core0, rows0, depth, 2)
        small = ((4, G3, c3, v3a, v3b), (SUB, 1, b4, v4a, v4b), (16, 1, b5, v5a, v5b))
        after = ((b4, 1), (b5, 1), (b6, 0))
        for (stride, g, b, va, vb), (coarse, ghost) in zip(small, after):
            n = b.shape[0] - 2 * g
            _mirror(b, n, g)
            _sweep(b, va, b, stride, g, n)
            _mirror(va, n, g)
            _restrict(va, b, stride, tmp, g, coarse, ghost, n // 2, 0, 0, coarse.shape[1], 4)
        bottom()
        coarse, last_row = v6, COARSE - 1
        for stride, g, b, va, vb in reversed(small):
            n = b.shape[0] - 2 * g
            _prolong(coarse, va, stride, tmp, g, 1, n // 2, 0, 4, last_row)
            _mirror(va, n, g)
            _sweep(va, vb, b, stride, g, n)
            _mirror(vb, n, g)
            _sweep(vb, va, b, stride, g, n)
            _mirror(va, n, g)
            coarse, last_row = va, SUB - 1
        half = H // 2
        _prolong(v3a, v2a, 2, tmp, 0, G3 + n3 * zq - half, n3 + H, (r3 - 4) * yh, 2)
        _sweep(v2a, v2b, c2, 2, 2, c2.shape[0] - 4)
        _sweep(v2b, v2a, c2, 2, 2, c2.shape[0] - 4)
        _prolong(v2a, v1a, 1, tmp, 0, half, n2 + H, 4 * yh, 2)
        _sweep(v1a, v1b, c1, 1, 2, c1.shape[0] - 4)
        _sweep(v1b, v1a, c1, 1, 2, c1.shape[0] - 4)
        wait_v()
        reflect(u0, core0, depth, 2)
        _prolong0(v1a, u0, tmp, yh, depth, core0)
        for left in reversed(range(0, depth - 1 if more else depth, 2)):
            _sweep0(u0, u1, f, left + 1 + more, core0)
            _sweep0(u1, u0, f, left + more, core0)

    core_row = pl.multiple_of(SUB * yh, SUB)
    slot = new_slot()
    here, there = pl.ds(core0 * gx, core0), pl.ds(core0 * (1 - gx), core0)
    give = remote(u1.at[0, pl.ds(0, core0), pl.ds(0, rows0)], out.at[here], slot, to(gz, gy, 1 - gx))
    take = remote(u1.at[0, pl.ds(0, core0), pl.ds(0, rows0)], out.at[there], slot, to(gz, gy, 1 - gx))

    def unsplit(z):
        at, rows = pl.ds(H + z, PERMUTE), pl.ds(core_row, rows0)
        x = jnp.concatenate([u0[0, at, rows], u0[1, at, rows]], axis=-1)
        y = _split_dot(x.reshape(-1, 2 * LANES), merge).reshape(x.shape)
        low, high = y[..., :LANES], y[..., LANES:]
        out[pl.ds(core0 * gx + z, PERMUTE)] = jnp.where(gx == 0, low, high)
        u1[0, pl.ds(z, PERMUTE), pl.ds(0, rows0)] = jnp.where(gx == 0, high, low)

    _loop(0, core0, PERMUTE, unsplit)
    give.start()
    give.wait_send()
    take.wait_recv()


SLOTS = 80


def solution(mesh):
    spec = P(("batch", "gz"), "gy", "gx")

    def local(rhs, init, inv):
        def vm(*shape):
            return pltpu.VMEM(shape, F32)

        def level(planes, rows, *lead):
            return [vm(*lead, planes, rows, LANES), vm(planes, rows, LANES), vm(planes, rows, LANES)]

        nz, ny = init.shape[0] // 2, init.shape[1]
        scratch = [vm(2, nz + 2 * H, ny + SUB, LANES)] * 3
        for l in (1, 2):
            scratch += level((nz >> l) + 2 * H, (ny >> l) + SUB, CYCLES)
        scratch += level(nz // 2 + 2 * G3, nz // 2, CYCLES)
        scratch += level(nz // 4 + 2, nz // 4) + level(nz // SUB + 2, SUB)
        scratch += [vm(COARSE, SUB, LANES), vm(COARSE + 2, SUB, LANES), vm(16, ny + 3 * SUB, LANES)]
        sems = pltpu.SemaphoreType.DMA((SLOTS,))
        call = pl.pallas_call(
            _kernel,
            out_shape=pltpu.VMEM(init.shape, F32),
            in_specs=[pl.BlockSpec(memory_space=pl.ANY)] * 2 + [pl.BlockSpec(memory_space=pltpu.VMEM)],
            out_specs=pl.BlockSpec(memory_space=pltpu.VMEM),
            scratch_shapes=scratch + [sems] * 3,
            compiler_params=pltpu.CompilerParams(
                collective_id=0, has_side_effects=True, vmem_limit_bytes=54 * 2**20
            ),
            name="vcycles",
        )
        return call(init, rhs, inv)

    return jax.shard_map(local, mesh=mesh, in_specs=(spec, spec, P()), out_specs=spec, check_vma=False)
```

```python
import functools

import jax
import jax.numpy as jnp
from jax import lax
from jax.experimental import pallas as pl
from jax.experimental.pallas import tpu as pltpu
from jax.sharding import PartitionSpec as P

MESH = pl.DeviceIdType.MESH
F32 = jnp.float32
NINTH = 1.0 / 9.0
H = 6
G3 = 4
CYCLES = 2
DU, DF, DV = 3, 4, 5
SUB, LANES = 8, 128
NEAR, FAR = 0.75, 0.25
COARSE = 4
PACK = 4
VREGS = 72
PERMUTE = 16
BLOCK0 = 72
BLOCK1 = 136
BLOCKP = 64


def _loop(lo, count, step, body):
    assert count % step == 0

    def run(i, carry):
        body(lo + i * step)
        return carry

    if count == step:
        body(lo)
    else:
        lax.fori_loop(0, count // step, run, 0)


def _iota(shape, axis):
    return lax.broadcasted_iota(jnp.int32, shape, len(shape) + axis)


def _ysum(load, lo, n, total, v, last_row=7):
    sub = _iota((v.shape[0], SUB, LANES), -2)
    if lo == 0:
        ym = jnp.where(sub == 0, -v[:, :SUB], pltpu.roll(v[:, :SUB], 1, 1))
        if n > SUB:
            ym = jnp.concatenate([ym, load(7, n - SUB)], axis=1)
    else:
        ym = load(lo - 1, n)
    if lo + n == total:
        yp = jnp.where(sub == last_row, -v[:, n - SUB :], pltpu.roll(v[:, n - SUB :], 7, 1))
        if n > SUB:
            yp = jnp.concatenate([load(lo + 1, n - SUB), yp], axis=1)
    else:
        yp = load(lo + 1, n)
    return ym + yp


def _blocks(total, size):
    return [(lo, min(size, total - lo)) for lo in range(0, total, size)]


def _planes0(src, f, z, u, emit, resid):
    total = src.shape[2]
    at, down, up = pl.ds(z, u), pl.ds(z - 1, u), pl.ds(z + 1, u)
    for lo, n in _blocks(total, BLOCK0):
        lane = _iota((u, n, LANES), -1)
        ends = (lane == 0, lane == 127)
        if resid:
            coef = tuple(jnp.where(e, 7.0, 6.0) for e in ends)
        else:
            coef = tuple(jnp.where(e, 2.0 * NINTH, 3.0 * NINTH) for e in ends)
        rows = pl.ds(lo, n)
        v = (src[0, at, rows, :], src[1, at, rows, :])
        x = (
            v[1] + jnp.where(ends[0], 0.0, pltpu.roll(v[1], 1, 2)),
            v[0] + jnp.where(ends[1], 0.0, pltpu.roll(v[0], 127, 2)),
        )
        for p in range(2):
            ys = _ysum(lambda r, m: src[p, at, pl.ds(r, m), :], lo, n, total, v[p])
            zs = src[p, down, rows, :] + src[p, up, rows, :]
            s = (x[p] + ys) + zs
            d = NINTH * (s - coef[p] * v[p]) if resid else coef[p] * v[p] + NINTH * s
            emit(p, lo, n, d + f[p, at, rows, :])


def _sweep0(src, dst, f, depth, n):
    lo, count = H - depth, n + 2 * depth
    step = min((17, 16, 14, 12, 11), key=lambda u: -(-count // u) * u)
    whole = -(-count // step) * step
    lo -= (whole - count) // 2

    def body(z):
        def emit(p, row, m, value):
            dst[p, pl.ds(z, step), pl.ds(row, m), :] = value

        _planes0(src, f, z, step, emit, False)

    _loop(lo, whole, step, body)


def _pairs(value):
    value = value.reshape(value.shape[0] // 2, 2, *value.shape[1:])
    return value[:, 0] + value[:, 1]


def _restrict0(src, f, coarse, tmp, yh, n):
    half = (src.shape[2] - SUB) // 2
    step = 4

    def body(zc):
        acc = {}

        def emit(p, lo, m, value):
            acc[lo] = (acc[lo][0] + value, m) if lo in acc else (value, m)

        _planes0(src, f, H + 2 * zc, 2 * step, emit, True)
        for lo, (value, m) in acc.items():
            tmp[pl.ds(0, step), pl.ds(lo, m), :] = _pairs(value)
        even = tmp[pl.ds(0, step), pl.ds(SUB * yh, half, stride=2), :]
        odd = tmp[pl.ds(0, step), pl.ds(SUB * yh + 1, half, stride=2), :]
        coarse[pl.ds(H + zc, step), pl.ds(pl.multiple_of(SUB * yh, SUB), half), :] = 0.5 * (even + odd)

    _loop(0, n // 2, step, body)


def _prolong_zy(coarse, zc, u, start, n, at_top, at_end, last_row=7):
    sub = _iota((2 * u, SUB, LANES), -2)

    def load(r, m):
        rows = pl.ds(r, m)
        c = NEAR * coarse[pl.ds(zc, u), rows, :]
        low = c + FAR * coarse[pl.ds(zc - 1, u), rows, :]
        high = c + FAR * coarse[pl.ds(zc + 1, u), rows, :]
        return jnp.stack([low, high], axis=1).reshape(2 * u, m, LANES)

    c = load(start, n)
    if at_top:
        cm = jnp.where(sub == 0, -c[:, :SUB], pltpu.roll(c[:, :SUB], 1, 1))
        if n > SUB:
            cm = jnp.concatenate([cm, load(start + 7, n - SUB)], axis=1)
    else:
        cm = load(start - 1, n)
    if at_end:
        cp = jnp.where(sub == last_row, -c[:, n - SUB :], pltpu.roll(c[:, n - SUB :], 7, 1))
        if n > SUB:
            cp = jnp.concatenate([load(start + 1, n - SUB), cp], axis=1)
    else:
        cp = load(start + 1, n)
    return NEAR * c + FAR * cm, NEAR * c + FAR * cp


def _y_parts(rows, offset, block):
    parts = []
    whole = rows // 16 * SUB
    for lo, n in _blocks(whole, block):
        end = lo + n == whole and rows % 16 == 0
        parts.append((offset + lo, n, 2 * lo, 2 * n, lo == 0, end, 0))
    if rows % 16:
        if rows == SUB:
            parts.append((offset, SUB, 0, SUB, True, True, 0))
        else:
            parts.append((offset + whole - 4, SUB, rows - SUB, SUB, False, True, SUB))
    return parts


def _prolong0(coarse, u, tmp, yh, depth, n):
    parts = _y_parts(u.shape[2], 4 * yh, BLOCKP)
    step = 2
    around = (depth + 1) // 2

    def body(zc):
        fine_at = pl.ds(H + 2 * (zc - H), 2 * step)
        for start, m, fine, count, top, end, skip in parts:
            pair = _prolong_zy(coarse, zc, step, start, m, top, end)
            lane = _iota((2 * step, m, LANES), -1)
            for parity in range(2):
                edge = lane == (0 if parity == 0 else 127)
                slots = pl.ds(2 * step * parity, 2 * step)
                for yc, c in enumerate(pair):
                    side = jnp.where(edge, -c, pltpu.roll(c, 1 if parity == 0 else 127, 2))
                    e = NEAR * c + FAR * side
                    if skip:
                        tmp[slots, pl.ds(fine - skip + yc, m, stride=2), :] = e
                    else:
                        u[parity, fine_at, pl.ds(fine + yc, m, stride=2), :] += e
                if skip:
                    u[parity, fine_at, pl.ds(fine, count), :] += tmp[slots, pl.ds(fine, count), :]

    _loop(H - around, n // 2 + 2 * around, step, body)


def _planes(src, b, z, u, stride, emit, resid):
    total = src.shape[1]
    at = pl.ds(z, u)
    for lo, n in _blocks(total, BLOCK1):
        lane = _iota((u, n, LANES), -1)
        first, last = lane < stride, lane >= LANES - stride
        edge = jnp.where(first, 1.0, 0.0) + jnp.where(last, 1.0, 0.0)
        coef = 6.0 + edge if resid else (3.0 - edge) * NINTH
        rows = pl.ds(lo, n)
        v = src[at, rows, :]
        x = jnp.where(first, 0.0, pltpu.roll(v, stride, 2)) + jnp.where(last, 0.0, pltpu.roll(v, LANES - stride, 2))
        ys = _ysum(lambda r, m: src[at, pl.ds(r, m), :], lo, n, total, v)
        s = (x + ys) + (src[pl.ds(z - 1, u), rows, :] + src[pl.ds(z + 1, u), rows, :])
        d = NINTH * (s - coef * v) if resid else coef * v + NINTH * s
        emit(lo, n, d + b[at, rows, :])


def _sweep(src, dst, b, stride, lo, count):
    tiles = src.shape[1] // SUB
    step = max(u for u in range(1, count + 1) if count % u == 0 and u * tiles <= VREGS)

    def body(z):
        def emit(row, m, value):
            dst[pl.ds(z, step), pl.ds(row, m), :] = value

        _planes(src, b, z, step, stride, emit, False)

    _loop(lo, count, step, body)


def _restrict(src, b, stride, tmp, fine_lo, coarse, coarse_lo, count, fine_row, coarse_row, rows, step):
    def body(i):
        acc = {}

        def emit(lo, m, value):
            acc[lo] = (value, m)

        _planes(src, b, fine_lo + 2 * i, 2 * step, stride, emit, True)
        slots = pl.ds(0, step)
        for lo, (value, m) in acc.items():
            tmp[slots, pl.ds(lo, m), :] = _pairs(value)
        s = tmp[slots, pl.ds(fine_row, rows, stride=2), :] + tmp[slots, pl.ds(fine_row + 1, rows, stride=2), :]
        s = 0.5 * (s + pltpu.roll(s, LANES - stride, 2))
        row = coarse_row if isinstance(coarse_row, int) else pl.multiple_of(coarse_row, SUB)
        coarse[pl.ds(coarse_lo + i, step), pl.ds(row, rows), :] = s

    _loop(0, count, step, body)


def _prolong(coarse, v, stride, tmp, fine_lo, coarse_lo, count, offset, step, last_row=7):
    parts = _y_parts(v.shape[1], offset, BLOCKP)

    def body(i):
        fine_at = pl.ds(fine_lo + 2 * i, 2 * step)
        slots = pl.ds(0, 2 * step)
        for start, m, fine, n, top, end, skip in parts:
            lane = _iota((2 * step, m, LANES), -1)
            is_high = jnp.bitwise_and(lane, stride) != 0
            edge = (is_high & (lane >= LANES - 2 * stride)) | (jnp.logical_not(is_high) & (lane < 2 * stride))
            for yc, c in enumerate(_prolong_zy(coarse, coarse_lo + i, step, start, m, top, end, last_row)):
                own = jnp.where(is_high, pltpu.roll(c, stride, 2), c)
                side = jnp.where(is_high, pltpu.roll(c, LANES - stride, 2), pltpu.roll(c, 2 * stride, 2))
                side = jnp.where(edge, -own, side)
                tmp[slots, pl.ds(fine - skip + yc, m, stride=2), :] = NEAR * own + FAR * side
            v[fine_at, pl.ds(fine, n), :] += tmp[slots, pl.ds(fine, n), :]

    _loop(0, count, step, body)


def _mirror(ref, planes, ghost):
    def fill(k, carry=0):
        ref[ghost - 1 - k] = -ref[ghost + k]
        ref[ghost + planes + k] = -ref[ghost + planes - 1 - k]
        return carry

    if ghost == 1:
        fill(0)
    else:
        lax.fori_loop(0, ghost, fill, 0)


def _split_dot(x, m, left=False):
    hi = x.astype(jnp.bfloat16).astype(F32)
    rest = x - hi
    mid = rest.astype(jnp.bfloat16).astype(F32)
    low = rest - mid
    dot = functools.partial(jnp.dot, preferred_element_type=F32)
    if left:
        return (dot(m, hi) + dot(m, mid)) + dot(m, low)
    return (dot(hi, m) + dot(mid, m)) + dot(low, m)


def _kernel(u_in, f_in, inv, out, u0, u1, f, b1, v1a, v1b, b2, v2a, v2b, b3, v3a, v3b, p3, b4, v4a, v4b, b5, v5a, v5b,
            b6, v6, tmp, send, recv, local):
    gz, gy, gx = (lax.axis_index(name) for name in ("gz", "gy", "gx"))
    zq, yh = 2 * gz + gx, gy
    core0, rows0 = u0.shape[1] - 2 * H, u0.shape[2] - SUB
    n1, n2, n3 = core0 // 2, core0 // 4, core0 // SUB
    r1, r2, r3 = rows0 // 2, rows0 // 4, rows0 // SUB
    counter = [0]

    def to(z, y, x):
        return {"gz": z, "gy": y, "gx": x}

    def remote(src, dst, slot, device):
        return pltpu.make_async_remote_copy(src_ref=src, dst_ref=dst, send_sem=send.at[slot], recv_sem=recv.at[slot],
                                            device_id=device, device_id_type=MESH)

    def new_slot():
        counter[0] += 1
        return counter[0] - 1

    barrier = pltpu.get_barrier_semaphore()
    others = [(a, b, c) for a in range(2) for b in range(2) for c in range(2) if a + b + c]
    for a, b, c in others:
        pl.semaphore_signal(barrier, inc=1, device_id=to(lax.rem(gz + a, 2), lax.rem(gy + b, 2), lax.rem(gx + c, 2)),
                            device_id_type=MESH)
    pl.semaphore_wait(barrier, len(others))

    def seam(m, d, start):
        below = SUB - d
        return (1 - yh) * (m - d) + yh * start, (1 - yh) * below + yh * m, yh * below + (1 - yh) * m

    def scatter(brick, window, d, lsem):
        waits = []
        n = core0 + d

        def mine(t):
            return brick.at[pl.ds(t * (core0 - d), n)]

        def place(half, t, row, count):
            return window.at[half, pl.ds(H - t * d, n), pl.ds(row, count)]

        row_src, row_dst, row_in = seam(rows0, d, 0)
        core_row = pl.multiple_of(SUB * gy, SUB)
        own = pltpu.make_async_copy(mine(gx), place(gx, gx, core_row, rows0), local.at[lsem])
        own.start()
        waits.append(own.wait)
        t_far = 1 - gz
        z_src = (1 - gz) * (LANES - d)
        z_dst = jnp.where(gz == 0, H - d, H + core0)
        z_in = jnp.where(gz == 0, H + core0, H - d)
        inner = gx == 1 - gz
        slots = {(kind, s): new_slot() for kind in ("z", "d") for s in range(2)}
        for s in range(2):
            cz = remote(brick.at[pl.ds(z_src, d)], window.at[s, pl.ds(z_dst, d), pl.ds(core_row, rows0)],
                        slots["z", s], to(1 - gz, gy, 1 - t_far))
            cd = remote(brick.at[pl.ds(z_src, d), pl.ds(row_src, d)], window.at[s, pl.ds(z_dst, d), pl.ds(row_dst, d)],
                        slots["d", s], to(1 - gz, 1 - gy, 1 - t_far))
            rz = remote(brick.at[pl.ds(z_src, d)], window.at[s, pl.ds(z_in, d), pl.ds(core_row, rows0)],
                        slots["z", s], to(1 - gz, gy, 1 - t_far))
            rd = remote(brick.at[pl.ds(z_src, d), pl.ds(row_src, d)], window.at[s, pl.ds(z_in, d), pl.ds(row_in, d)],
                        slots["d", s], to(1 - gz, 1 - gy, 1 - t_far))

            @pl.when(gx == s)
            def _():
                cz.start()
                cd.start()

            def wait(cz=cz, cd=cd, rz=rz, rd=rd, s=s):
                @pl.when(gx == s)
                def _():
                    cz.wait_send()
                    cd.wait_send()

                @pl.when(inner)
                def _():
                    rz.wait_recv()
                    rd.wait_recv()

            waits.append(wait)
        slots = {(s, t): new_slot() for s in range(2) for t in range(2)}
        for s in range(2):
            for t in range(2):
                cy = remote(brick.at[pl.ds(t * (core0 - d), n), pl.ds(row_src, d)], place(s, t, row_dst, d),
                            slots[s, t], to(gz, 1 - gy, t))
                ry = remote(brick.at[pl.ds(t * (core0 - d), n), pl.ds(row_src, d)], place(s, t, row_in, d),
                            slots[s, t], to(gz, 1 - gy, t))

                @pl.when(gx == s)
                def _():
                    cy.start()

                def wait(cy=cy, ry=ry, s=s, t=t):
                    @pl.when(gx == s)
                    def _():
                        cy.wait_send()

                    @pl.when(gx == t)
                    def _():
                        ry.wait_recv()

                waits.append(wait)
        slot = new_slot()
        cp = remote(mine(1 - gx), place(gx, 1 - gx, core_row, rows0), slot, to(gz, gy, 1 - gx))
        rp = remote(mine(gx), place(1 - gx, gx, core_row, rows0), slot, to(gz, gy, 1 - gx))
        cp.start()

        def wait():
            cp.wait_send()
            rp.wait_recv()

        waits.append(wait)
        return waits

    def reflect(ref, n, d, lead):
        def fill(dst, src):
            def step(k, carry):
                for p in range(lead):
                    r = ref.at[p] if lead > 1 else ref
                    r[dst(k)] = -r[src(k)]
                return carry

            lax.fori_loop(0, d, step, 0)

        @pl.when(zq == 0)
        def _():
            fill(lambda k: H - 1 - k, lambda k: H + k)

        @pl.when(zq == 3)
        def _():
            fill(lambda k: H + n + k, lambda k: H + n - 1 - k)

    def exchange(ref, n, m, d, lead):
        pre = (slice(None),) if lead > 1 else ()

        def at(z, dz, row, dr):
            return ref.at[pre + (pl.ds(z, dz), pl.ds(row, dr))]

        core_row = pl.multiple_of(SUB * yh, SUB)
        row_src, row_dst, row_in = seam(m, d, SUB)
        waits = []
        slot = new_slot()
        across = remote(at(H, n, row_src, d), at(H, n, row_dst, d), slot, to(gz, 1 - gy, gx))
        arrive = remote(at(H, n, row_src, d), at(H, n, row_in, d), slot, to(gz, 1 - gy, gx))
        jobs = []
        for up in (False, True):
            qz = jnp.minimum(gz + gx, 1) if up else jnp.maximum(gz + gx - 1, 0)
            qx = 1 - gx
            z_src = H + n - d if up else H
            z_dst = H - d if up else H + n
            z_in = H - d if up else H + n
            sends = zq < 3 if up else zq > 0
            takes = zq > 0 if up else zq < 3
            sz, sd = new_slot(), new_slot()
            cz = remote(at(z_src, d, core_row, m), at(z_dst, d, core_row, m), sz, to(qz, gy, qx))
            cd = remote(at(z_src, d, row_src, d), at(z_dst, d, row_dst, d), sd, to(qz, 1 - gy, qx))
            rz = remote(at(z_src, d, core_row, m), at(z_in, d, core_row, m), sz, to(qz, gy, qx))
            rd = remote(at(z_src, d, row_src, d), at(z_in, d, row_in, d), sd, to(qz, 1 - gy, qx))
            jobs.append((sends, takes, cz, cd, rz, rd))
        for sends, _, cz, cd, _, _ in jobs:

            @pl.when(sends)
            def _():
                cd.start()
                cz.start()

        across.start()

        def wait():
            across.wait_send()
            arrive.wait_recv()
            for sends, takes, cz, cd, rz, rd in jobs:

                @pl.when(sends)
                def _():
                    cz.wait_send()
                    cd.wait_send()

                @pl.when(takes)
                def _():
                    rz.wait_recv()
                    rd.wait_recv()

        waits.append(wait)
        return wait

    waits_u = scatter(u_in, u0, DU, 0)
    waits_f = scatter(f_in, f, DF, 1)

    col = lax.broadcasted_iota(jnp.int32, (256, 256), 1)
    row = lax.broadcasted_iota(jnp.int32, (256, 256), 0)
    split = (row == 2 * jnp.bitwise_and(col, 127) + lax.shift_right_logical(col, 7)).astype(F32)
    merge = (col == 2 * jnp.bitwise_and(row, 127) + lax.shift_right_logical(row, 7)).astype(F32)
    def lanes(shape, axis, sign):
        cell = lax.broadcasted_iota(jnp.int32, shape, 1 - axis)
        spot = lax.broadcasted_iota(jnp.int32, shape, axis)
        z = lax.shift_right_logical(cell, 4)
        y = jnp.bitwise_and(lax.shift_right_logical(cell, 2), 3)
        x = jnp.bitwise_and(cell, 3)
        return (spot == jnp.bitwise_and(32 * x + sign * (4 * z + y), 127)).astype(F32)

    table = _split_dot(_split_dot(inv[...], lanes((64, LANES), 1, -1)), lanes((LANES, 64), 0, 1), left=True) * (9.0 * 16.0)

    for wait in waits_u:
        wait()

    def permute(ref, m, scale, lo, count, dst):
        step = max(u for u in range(1, PERMUTE + 1) if count % u == 0)

        def body(z):
            at = pl.ds(z, step)
            x = jnp.concatenate([ref[0, at], ref[1, at]], axis=-1)
            y = _split_dot(x.reshape(-1, 2 * LANES), m).reshape(x.shape)
            if scale is not None:
                y = y * scale
            dst[0, at] = y[..., :LANES]
            dst[1, at] = y[..., LANES:]

        _loop(lo, count, step, body)

    reflect(u0, core0, DU, 2)
    permute(u0, split, None, H - DU, core0 + 2 * DU, u0)
    for wait in waits_f:
        wait()
    reflect(f, core0, DF, 2)
    permute(f, split, NINTH / 65536.0, H - DF, core0 + 2 * DF, f)

    def bottom():
        lane, sub = _iota(v6.shape[1:], -1), _iota(v6.shape[1:], -2)
        valid = jnp.bitwise_and(lane, 31) == 0
        total = jnp.zeros(v6.shape[1:], F32)
        for i in range(COARSE * COARSE):
            z, y = divmod(i, COARSE)
            total = total + pltpu.roll(jnp.where(valid & (sub == y), b6[z], 0.0), i, 1)
        for shift in (4, 2, 1):
            total = total + pltpu.roll(total, shift, 0)
        e6 = jnp.dot(total, table, precision=lax.Precision.HIGHEST, preferred_element_type=F32)
        for z in range(COARSE):
            plane = e6
            for y in range(COARSE):
                plane = jnp.where(sub == y, pltpu.roll(e6, COARSE * z + y, 1), plane)
            v6[1 + z] = plane
        _mirror(v6, COARSE, 1)

    for cycle in range(CYCLES):
        c1, c2, c3 = b1.at[cycle], b2.at[cycle], b3.at[cycle]
        more = cycle + 1 < CYCLES
        if cycle == 0:
            _sweep0(u0, u1, f, 2, core0)
            _sweep0(u1, u0, f, 1, core0)
        _restrict0(u0, f, c1, tmp, yh, core0)
        wait_b1 = exchange(c1, n1, r1, H, 1)
        wait_b1()
        reflect(c1, n1, H, 1)
        _sweep(c1, v1a, c1, 1, 1, c1.shape[0] - 2)
        _restrict(v1a, c1, 1, tmp, H, c2, H, n2, SUB * yh, SUB * yh, r2, 4)
        wait_b2 = exchange(c2, n2, r2, H, 1)
        wait_b2()
        reflect(c2, n2, H, 1)
        _sweep(c2, v2a, c2, 2, 1, c2.shape[0] - 2)
        _restrict(v2a, c2, 2, tmp, H, c3, G3 + n3 * zq, n3, SUB * yh, r3 * yh, r3, 4)
        for i in range(n3 // PACK):
            at = pl.multiple_of(r3 * yh, SUB)
            lane = jnp.bitwise_and(_iota((r3, LANES), -1), PACK - 1)
            row = [c3[G3 + n3 * zq + PACK * i + k, pl.ds(at, r3), :] for k in range(PACK)]
            packed = row[0]
            for k in range(1, PACK):
                packed = jnp.where(lane == k, pltpu.roll(row[k], k, 1), packed)
            p3[cycle, n3 // PACK * zq + i, pl.ds(at, r3), :] = packed
        waits3 = []

        def block(z, y, x):
            return p3.at[cycle, pl.ds(n3 // PACK * (2 * z + x), n3 // PACK), pl.ds(pl.multiple_of(r3 * y, SUB), r3)]

        for a, b, c in others:
            z, y, x = lax.rem(gz + a, 2), lax.rem(gy + b, 2), lax.rem(gx + c, 2)
            slot = new_slot()
            src = block(gz, gy, gx)
            give = remote(src, src, slot, to(z, y, x))
            take = remote(src, block(z, y, x), slot, to(z, y, x))
            give.start()
            waits3.append((give, take))
        for give, take in waits3:
            give.wait_send()
            take.wait_recv()
        for k in range(PACK):
            for i in range(p3.shape[1]):
                packed = p3[cycle, i]
                c3[G3 + PACK * i + k] = pltpu.roll(packed, LANES - k, 1) if k else packed
        depth = DV if more else 2
        wait_v = exchange(u0, core0, rows0, depth, 2)
        small = ((4, G3, c3, v3a, v3b), (SUB, 1, b4, v4a, v4b), (16, 1, b5, v5a, v5b))
        after = ((b4, 1), (b5, 1), (b6, 0))
        for (stride, g, b, va, vb), (coarse, ghost) in zip(small, after):
            n = b.shape[0] - 2 * g
            _mirror(b, n, g)
            _sweep(b, va, b, stride, g, n)
            _mirror(va, n, g)
            _restrict(va, b, stride, tmp, g, coarse, ghost, n // 2, 0, 0, coarse.shape[1], 4)
        bottom()
        coarse, last_row = v6, COARSE - 1
        for stride, g, b, va, vb in reversed(small):
            n = b.shape[0] - 2 * g
            _prolong(coarse, va, stride, tmp, g, 1, n // 2, 0, 4, last_row)
            _mirror(va, n, g)
            _sweep(va, vb, b, stride, g, n)
            _mirror(vb, n, g)
            _sweep(vb, va, b, stride, g, n)
            _mirror(va, n, g)
            coarse, last_row = va, SUB - 1
        half = H // 2
        _prolong(v3a, v2a, 2, tmp, 0, G3 + n3 * zq - half, n3 + H, (r3 - 4) * yh, 2)
        _sweep(v2a, v2b, c2, 2, 2, c2.shape[0] - 4)
        _sweep(v2b, v2a, c2, 2, 2, c2.shape[0] - 4)
        _prolong(v2a, v1a, 1, tmp, 0, half, n2 + H, 4 * yh, 2)
        _sweep(v1a, v1b, c1, 1, 2, c1.shape[0] - 4)
        _sweep(v1b, v1a, c1, 1, 2, c1.shape[0] - 4)
        wait_v()
        reflect(u0, core0, depth, 2)
        _prolong0(v1a, u0, tmp, yh, depth, core0)
        for left in reversed(range(0, depth - 1 if more else depth, 2)):
            _sweep0(u0, u1, f, left + 1 + more, core0)
            _sweep0(u1, u0, f, left + more, core0)

    core_row = pl.multiple_of(SUB * yh, SUB)
    slot = new_slot()
    here, there = pl.ds(core0 * gx, core0), pl.ds(core0 * (1 - gx), core0)
    give = remote(u1.at[0, pl.ds(0, core0), pl.ds(0, rows0)], out.at[here], slot, to(gz, gy, 1 - gx))
    take = remote(u1.at[0, pl.ds(0, core0), pl.ds(0, rows0)], out.at[there], slot, to(gz, gy, 1 - gx))

    def unsplit(z):
        at, rows = pl.ds(H + z, PERMUTE), pl.ds(core_row, rows0)
        x = jnp.concatenate([u0[0, at, rows], u0[1, at, rows]], axis=-1)
        y = _split_dot(x.reshape(-1, 2 * LANES), merge).reshape(x.shape)
        low, high = y[..., :LANES], y[..., LANES:]
        out[pl.ds(core0 * gx + z, PERMUTE)] = jnp.where(gx == 0, low, high)
        u1[0, pl.ds(z, PERMUTE), pl.ds(0, rows0)] = jnp.where(gx == 0, high, low)

    _loop(0, core0, PERMUTE, unsplit)
    give.start()
    give.wait_send()
    take.wait_recv()


SLOTS = 80


def solution(mesh):
    spec = P(("batch", "gz"), "gy", "gx")

    def local(rhs, init, inv):
        def vm(*shape):
            return pltpu.VMEM(shape, F32)

        def level(planes, rows, *lead):
            return [vm(*lead, planes, rows, LANES), vm(planes, rows, LANES), vm(planes, rows, LANES)]

        nz, ny = init.shape[0] // 2, init.shape[1]
        scratch = [vm(2, nz + 2 * H, ny + SUB, LANES)] * 3
        for l in (1, 2):
            scratch += level((nz >> l) + 2 * H, (ny >> l) + SUB, CYCLES)
        scratch += level(nz // 2 + 2 * G3, nz // 2, CYCLES)
        scratch += [vm(CYCLES, nz // (2 * PACK), nz // 2, LANES)]
        scratch += level(nz // 4 + 2, nz // 4) + level(nz // SUB + 2, SUB)
        scratch += [vm(COARSE, SUB, LANES), vm(COARSE + 2, SUB, LANES), vm(16, ny + 3 * SUB, LANES)]
        sems = pltpu.SemaphoreType.DMA((SLOTS,))
        call = pl.pallas_call(
            _kernel,
            out_shape=pltpu.VMEM(init.shape, F32),
            in_specs=[pl.BlockSpec(memory_space=pl.ANY)] * 2 + [pl.BlockSpec(memory_space=pltpu.VMEM)],
            out_specs=pl.BlockSpec(memory_space=pltpu.VMEM),
            scratch_shapes=scratch + [sems] * 3,
            compiler_params=pltpu.CompilerParams(
                collective_id=0, has_side_effects=True, vmem_limit_bytes=54 * 2**20
            ),
            name="vcycles",
        )
        return call(init, rhs, inv)

    return jax.shard_map(local, mesh=mesh, in_specs=(spec, spec, P()), out_specs=spec, check_vma=False)
```
